32 devices in a mesh: row: 4 (over y, core), col: 8 (over z, x).
Axes of the slice: x: 2, y: 2, z: 4, core: 2. Of those that a mesh axis runs over, the one named last changes fastest.
Arguments:
- amplitudes: float32 [48, 256, 1024], P('col', None, 'row'), may hold values from -6 to 6
- interaction: float32 [8192, 8192], P('row', 'col'), may hold values from -0.5 to 0.5, as said below
- tile_counts: int32 [8], replicated, may hold values from 2 to 6, as said below
- tile_block: int32 [48], replicated, may hold values from -1 to 31, as said below
- recouple_sign: int32 [48], replicated, may hold values from 0 to 1
- orbit_perm: int32 [48, 256], replicated, may hold values from 0 to 255, each once within a row
- particle_energy: float32 [48, 256], P('col'), may hold values from -2 to 2
Outputs:
- sigma: float32 [48, 256, 1024], P('col', None, 'row')
The draws below stay inside these ranges and needn't reach their ends.
Inputs may be any that keep to these rules, and one draw needn't show every extreme that they name: Owner c holds its live tiles in its first tile_counts[c] slots; the counts sum to 32, and some owner holds 6. `tile_block`: live slots map one to one onto the 32 cross-channel tiles, and slots that are not live hold -1; two live tiles of one owner never lie in the same aligned group of 4 cross-channel tiles. interaction equals its transpose.
All inputs are finite; a program needn't handle non-finite values.
Results may differ from the reference program's by a relative error of at most 0.000061.
Values sent between devices are 32-bit elements; how exact they have to be, the bound alone decides.
No kernel may reach another device: no remote copies, remote signals or barrier semaphores. Data moves between devices by JAX's collectives and lax.ppermute only.
A program may use at most 128 MiB of HBM per device.

```python
import jax
import jax.numpy as jnp
from jax import lax

TILE = 256
HCOLS = 1024
BLOCKS_DEV = 4
SLOTS = 6
BLOCKS = 32
ORDER = 8192
N_COL = 8


def shared_layout(key):
    folded = jax.random.fold_in(key, 11)
    key_pair, key_size, key_slot, key_target, key_within = jax.random.split(folded, 5)
    pairing = jax.random.permutation(key_pair, N_COL)
    spare_room = SLOTS - BLOCKS_DEV
    shifts = jax.random.randint(key_size, (N_COL // 2,), 0, spare_room + 1)
    shifts = shifts.at[0].set(spare_room)
    change = jnp.zeros((N_COL,), jnp.int32).at[pairing[0::2]].set(shifts).at[pairing[1::2]].set(-shifts)
    counts = (BLOCKS_DEV + change).astype(jnp.int32)
    starts = jnp.cumsum(counts) - counts
    slot_subkeys = jax.random.split(key_slot, N_COL)
    scramble = jax.vmap(lambda subkey: jax.random.permutation(subkey, SLOTS))(slot_subkeys)
    slot_ids = jnp.arange(SLOTS, dtype=jnp.int32)[None, :]
    is_live = slot_ids < counts[:, None]
    scores = jnp.where(is_live, scramble, SLOTS + slot_ids)
    ranking = jnp.argsort(jnp.argsort(scores, axis=1), axis=1)
    position = starts[:, None] + ranking
    relabel = jax.random.permutation(key_target, N_COL)
    target = relabel[position % N_COL]
    within_subkeys = jax.random.split(key_within, N_COL)
    within = jax.vmap(lambda subkey: jax.random.permutation(subkey, BLOCKS_DEV))(within_subkeys)
    blocks = target * BLOCKS_DEV + within[target, jnp.clip(position // N_COL, 0, BLOCKS_DEV - 1)]
    blocks = jnp.where(is_live, blocks, -1)
    return (counts, blocks.reshape(-1).astype(jnp.int32))


def draw_tile_counts(key, part):
    return shared_layout(key)[0]


def draw_tile_block(key, part):
    return shared_layout(key)[1]


def draw_interaction(key, part):
    key_main = jax.random.fold_in(jax.random.fold_in(key, 23), 0)
    normal_draw = jax.random.normal(key_main, (ORDER, ORDER), jnp.float32)
    symmetric = (normal_draw + normal_draw.T) * (0.5 / ORDER) ** 0.5
    return jnp.clip(symmetric, -0.5, 0.5)


def touch_ends(drawn, rng, low, high):
    longest = drawn.shape.index(max(drawn.shape))
    spots = []
    for shift in (0, 1):
        where = [jax.random.randint(jax.random.fold_in(rng, axis), (), 0, length) for axis, length in enumerate(drawn.shape)]
        where[longest] = (where[longest] + shift) % drawn.shape[longest]
        spots.append(tuple(where))
    return drawn.at[spots[0]].set(low).at[spots[1]].set(high)


def level_of(stream_key, shape, cuts, low, largest):
    factor_of, own = 1.0, jax.random.fold_in(stream_key, 6)
    for axis_at, blocks in cuts:
        heights = jnp.exp(jax.random.uniform(jax.random.fold_in(own, axis_at), (blocks,), jnp.float32, low / len(cuts), largest / len(cuts)))
        factor_of = factor_of * jnp.repeat(heights, shape[axis_at] // blocks).reshape([-1 if axis == axis_at else 1 for axis in range(len(shape))])
    return factor_of


def normal_values(own_key, extent, deviation, bound, pieces=(), kind=jnp.bfloat16):
    result = jax.random.normal(own_key, extent, jnp.float32) * deviation
    if len(pieces) > 0:
        result = level_of(own_key, extent, pieces, -0.22, 0.18) * result
    return jnp.clip(result, min=-bound, max=bound).astype(kind)


def setup_inputs(seed: int = 0) -> dict:
    splits = jax.random.split(jax.random.key(seed), 8)
    return {
        "amplitudes": normal_values(splits[0], (N_COL * SLOTS, TILE, HCOLS), 1.0, 6.0, ((0, 8), (2, 4)), jnp.float32),
        "interaction": draw_interaction(jax.random.fold_in(splits[7], 71), 0),
        "tile_counts": draw_tile_counts(jax.random.fold_in(splits[7], 71), 0),
        "tile_block": draw_tile_block(jax.random.fold_in(splits[7], 71), 0),
        "recouple_sign": touch_ends(jax.random.randint(splits[4], (N_COL * SLOTS,), 0, 2), jax.random.fold_in(splits[4], 1), 0, 1).astype(jnp.int32),
        "orbit_perm": jax.vmap(lambda own: jax.random.permutation(own, TILE))(jax.random.split(splits[5], (N_COL * SLOTS))).reshape((N_COL * SLOTS, TILE)).astype(jnp.int32),
        "particle_energy": jnp.clip(jax.random.uniform(splits[6], (N_COL * SLOTS, TILE), jnp.float32, -2.0, 2.0) * level_of(splits[6], (N_COL * SLOTS, TILE), ((0, 8),), -0.4, 0.0), -2.0, 2.0),
    }


def reorder_rows(tiles, orders):
    return jax.vmap(lambda single, ordering: jnp.take(single, ordering, axis=0))(tiles, orders)


def reference(amplitudes, interaction, tile_counts, tile_block, recouple_sign, orbit_perm, particle_energy):
    tile_total = amplitudes.shape[0]
    slot_ids = jnp.arange(tile_total, dtype=jnp.int32)
    owners = (slot_ids // SLOTS).astype(jnp.int32)
    is_live = (slot_ids % SLOTS) < jnp.take(tile_counts, owners)
    live_mask = is_live.astype(jnp.float32)[:, None, None]
    phases = (1 - 2 * recouple_sign).astype(jnp.float32)
    permuted = reorder_rows(amplitudes, orbit_perm) * phases[:, None, None]
    targets = jnp.where(is_live, tile_block, BLOCKS).astype(jnp.int32)
    cross_tiles = jnp.zeros((BLOCKS, TILE, HCOLS), jnp.float32).at[targets].set(permuted, mode="drop")
    image = jnp.dot(interaction, cross_tiles.reshape(ORDER, HCOLS), precision=lax.Precision.HIGHEST, preferred_element_type=jnp.float32)
    image = image.reshape(BLOCKS, TILE, HCOLS)
    picked = jnp.take(image, jnp.clip(tile_block, 0, BLOCKS - 1).astype(jnp.int32), axis=0)
    inverse = jnp.argsort(orbit_perm, axis=1).astype(jnp.int32)
    returned = reorder_rows(picked, inverse) * phases[:, None, None]
    sigma = (returned + particle_energy[:, :, None] * amplitudes) * live_mask
    return sigma
```

```python
import jax
import jax.numpy as jnp
from jax import lax
from jax.sharding import PartitionSpec as P


def xor_pairs(count, mask):
    return [(i, i ^ mask) for i in range(count)]


def halving_order(count):
    order, bit = [0], count // 2
    while bit >= 1:
        order = order + [entry ^ bit for entry in order]
        bit //= 2
    return order


def grid_of(columns):
    across = 1
    while across * across * 4 <= columns:
        across *= 2
    return columns // across, across


def exchange(tiles, count, use_permutes):
    if not use_permutes:
        return lax.all_to_all(tiles, "col", split_axis=0, concat_axis=0, tiled=True)
    me = lax.axis_index("col")
    parts = []
    for mask in range(count):
        piece = lax.dynamic_index_in_dim(tiles, me ^ mask, 0, keepdims=True)
        parts.append(piece if mask == 0 else lax.ppermute(piece, "col", xor_pairs(count, mask)))
    stacked = jnp.concatenate(parts, axis=0)
    return jnp.take(stacked, jnp.arange(count, dtype=jnp.int32) ^ me, axis=0)


def shards_of_line(own, depth, across):
    z = lax.axis_index("col") // across

    def hop(value, pairs):
        links = [(a * across + x, b * across + x) for a, b in pairs for x in range(across)]
        return lax.ppermute(value, "col", links)

    if depth != 4:
        out = [(own, z)]
        for step in range(1, depth):
            pairs = [(a, (a + step) % depth) for a in range(depth)]
            out.append((hop(own, pairs), (z + depth - step) % depth))
        return out
    inner = jnp.logical_or(z == 1, z == 2)
    from_pair = hop(own, [(0, 1), (1, 0), (2, 3), (3, 2)])
    from_middle = hop(own, [(1, 2), (2, 1)])
    from_far_end = hop(from_pair, [(1, 2), (2, 1)])
    outward_near = hop(from_middle, [(1, 0), (2, 3)])
    outward_far = hop(from_far_end, [(1, 0), (2, 3)])
    second = jnp.where(inner, from_middle, outward_near)
    third = jnp.where(inner, from_far_end, outward_far)
    low = z < 2
    return [
        (own, z),
        (from_pair, z ^ 1),
        (second, jnp.where(low, 2, 1)),
        (third, jnp.where(low, 3, 0)),
    ]


def local(
    amplitudes, interaction, tile_counts, tile_block, recouple_sign, orbit_perm, particle_energy
):
    column = lax.axis_index("col")
    row = lax.axis_index("row")
    columns = lax.axis_size("col")
    rows = lax.axis_size("row")
    depth, across = grid_of(columns)
    slots, tile_rows, narrow = amplitudes.shape
    row_blocks = interaction.shape[0] // tile_rows
    col_blocks = interaction.shape[1] // tile_rows
    tile_total = tile_block.shape[0]
    piece = tile_rows // columns
    order = halving_order(rows)

    slot_ids = jnp.arange(slots, dtype=jnp.int32)
    is_live = slot_ids < jnp.take(tile_counts, column)
    own_block = lax.dynamic_slice_in_dim(tile_block, column * slots, slots)
    own_phase = 1 - 2 * lax.dynamic_slice_in_dim(recouple_sign, column * slots, slots)
    own_perm = lax.dynamic_slice_in_dim(orbit_perm, column * slots, slots, 0)
    tile_ids = jnp.arange(tile_total, dtype=jnp.int32)

    def tiles_of(blocks):
        matches = tile_block[None, :] == blocks[:, None]
        return jnp.sum(jnp.where(matches, tile_ids[None, :], 0), axis=1)

    orbitals = jnp.arange(tile_rows, dtype=jnp.int32)
    recouple = jnp.where(
        own_perm[:, :, None] == orbitals[None, None, :], own_phase[:, None, None], 0
    ).astype(jnp.float32)

    permuted = jnp.einsum(
        "sjp,spn->sjn", recouple, amplitudes, precision=lax.Precision.HIGHEST
    )
    cut = permuted.reshape(slots, columns, piece, narrow).transpose(1, 0, 2, 3)
    cut = exchange(cut, columns, P1_PERMUTES).reshape(tile_total, piece, narrow)

    parts = {}
    for mask in order:
        blocks = (row ^ mask) * row_blocks + jnp.arange(row_blocks, dtype=jnp.int32)
        part = jnp.take(cut, tiles_of(blocks), axis=0)
        if mask:
            part = lax.ppermute(part, "row", xor_pairs(rows, mask))
        parts[mask] = part.reshape(row_blocks * piece, narrow)
    half = rows // 2
    shard = jnp.stack(
        [
            jnp.concatenate([parts[mask] for mask in order[:half]], axis=1),
            jnp.concatenate([parts[mask] for mask in order[half:]], axis=1),
        ]
    )

    weights = interaction.reshape(row_blocks, columns, piece, interaction.shape[1])
    x = column % across
    kept = sent = None
    for held, z in shards_of_line(shard, depth, across):
        for mask in range(across):
            if mask:
                links = [
                    (a * across + b, a * across + (b ^ mask))
                    for a in range(depth)
                    for b in range(across)
                ]
                got = lax.ppermute(held, "col", links)
            else:
                got = held
            weight = lax.dynamic_slice_in_dim(weights, z * across + (x ^ mask), 1, 1)
            weight = weight.reshape(row_blocks * piece, interaction.shape[1])

            def term(panel):
                return lax.dot_general(
                    weight,
                    panel,
                    (((0,), (0,)), ((), ())),
                    precision=lax.Precision.HIGH,
                    preferred_element_type=jnp.float32,
                )

            more_sent, more_kept = term(got[1]), term(got[0])
            sent = more_sent if sent is None else sent + more_sent
            kept = more_kept if kept is None else kept + more_kept

    bit = 1
    while True:
        arrived = lax.ppermute(sent, "row", xor_pairs(rows, bit))
        width = kept.shape[1]
        bit *= 2
        if bit >= rows:
            own = kept + arrived
            break
        sent = kept[:, width // 2 :] + arrived[:, width // 2 :]
        kept = kept[:, : width // 2] + arrived[:, : width // 2]

    here = own.reshape(col_blocks, tile_rows, narrow)
    my_blocks = column * col_blocks + jnp.arange(col_blocks, dtype=jnp.int32)
    owners = tiles_of(my_blocks) // slots
    peers = jnp.arange(columns, dtype=jnp.int32)
    choice = jnp.sum(
        jnp.where(
            owners[None, :] == peers[:, None], jnp.arange(col_blocks, dtype=jnp.int32)[None, :], 0
        ),
        axis=1,
    )
    home = exchange(jnp.take(here, choice, axis=0), columns, OUT_PERMUTES)
    source = jnp.clip(own_block // col_blocks, 0, columns - 1)
    picked = jnp.take(home, source, axis=0)
    returned = jnp.einsum("sjp,sjn->spn", recouple, picked, precision=lax.Precision.HIGHEST)
    sigma = returned + particle_energy[:, :, None] * amplitudes
    return jnp.where(is_live[:, None, None], sigma, 0.0)


P1_PERMUTES = False
OUT_PERMUTES = False


def solution(mesh):
    placed = (P("col", None, "row"), P("row", "col"), P(), P(), P(), P(), P("col", None))
    return jax.shard_map(
        local, mesh=mesh, in_specs=placed, out_specs=P("col", None, "row"), check_vma=False
    )
```

```python
import functools

import jax
import jax.numpy as jnp
from jax import lax
from jax.experimental import pallas as pl
from jax.experimental.pallas import tpu as pltpu
from jax.sharding import PartitionSpec as P


def xor_pairs(count, mask):
    return [(i, i ^ mask) for i in range(count)]


def halving_order(count):
    order, bit = [0], count // 2
    while bit >= 1:
        order = order + [entry ^ bit for entry in order]
        bit //= 2
    return order


def grid_of(columns):
    across = 1
    while across * across * 4 <= columns:
        across *= 2
    return columns // across, across


def exchange(tiles):
    return lax.all_to_all(tiles, "col", split_axis=0, concat_axis=0, tiled=True)


def after(value, *others):
    return lax.optimization_barrier((value, *others))[0]


class Line:
    def __init__(self, depth, across):
        self.depth, self.across = depth, across
        self.z = lax.axis_index("col") // across

    def hop(self, value, pairs):
        links = [
            (a * self.across + x, b * self.across + x) for a, b in pairs for x in range(self.across)
        ]
        return lax.ppermute(value, "col", links)

    def sources(self):
        z, depth = self.z, self.depth
        if depth != 4:
            return [z] + [(z + depth - step) % depth for step in range(1, depth)]
        low = z < 2
        return [z, z ^ 1, jnp.where(low, 2, 1), jnp.where(low, 3, 0)]

    def gather(self, own):
        z, depth = self.z, self.depth
        if depth != 4:
            out = [(own, z)]
            for step in range(1, depth):
                pairs = [(a, (a + step) % depth) for a in range(depth)]
                out.append((self.hop(own, pairs), (z + depth - step) % depth))
            return out
        inner, low = jnp.logical_or(z == 1, z == 2), z < 2
        from_pair = self.hop(own, [(0, 1), (1, 0), (2, 3), (3, 2)])
        from_middle = self.hop(own, [(1, 2), (2, 1)])
        from_far_end = self.hop(from_pair, [(1, 2), (2, 1)])
        outward_near = self.hop(from_middle, [(1, 0), (2, 3)])
        outward_far = self.hop(from_far_end, [(1, 0), (2, 3)])
        second = jnp.where(inner, from_middle, outward_near)
        third = jnp.where(inner, from_far_end, outward_far)
        return [
            (own, z),
            (from_pair, z ^ 1),
            (second, jnp.where(low, 2, 1)),
            (third, jnp.where(low, 3, 0)),
        ]


def halves(value):
    high = value.astype(jnp.bfloat16)
    return high, (value - high.astype(jnp.float32)).astype(jnp.bfloat16)


def weights_kernel(index, weight, high, low):
    del index
    rows = weight.shape[0] * weight.shape[2]
    high[0], low[0] = halves(weight[...].reshape(rows, weight.shape[3]).T)


def turned_weights(weights, index):
    groups, _, piece, height = weights.shape
    tile, count = min(512, height), index.shape[0]
    shape = jax.ShapeDtypeStruct((count, height, groups * piece), jnp.bfloat16)
    spec = pl.BlockSpec((1, tile, groups * piece), lambda k, m, index: (k, m, 0))
    return pl.pallas_call(
        weights_kernel,
        grid_spec=pltpu.PrefetchScalarGridSpec(
            num_scalar_prefetch=1,
            grid=(count, height // tile),
            in_specs=[
                pl.BlockSpec(
                    (groups, 1, piece, tile), lambda k, m, index: (0, index[k], 0, m)
                )
            ],
            out_specs=[spec, spec],
        ),
        out_shape=[shape, shape],
        cost_estimate=pl.CostEstimate(
            flops=20 * count * groups * piece * height * 100,
            bytes_accessed=8 * count * groups * piece * height,
            transcendentals=0,
        ),
        name="turned_weights",
    )(index, weights)


def product_kernel(count, has_start, splits, *refs):
    high, low, panels = refs[:count], refs[count : 2 * count], refs[2 * count : 3 * count]
    rest = refs[3 * count :]
    outs = rest[1:] if has_start else rest
    total = rest[0][...] if has_start else None

    def dot(a, b):
        return jnp.dot(a, b, preferred_element_type=jnp.float32)

    for w_high, w_low, panel in zip(high, low, panels):
        p_high, p_low = halves(panel[...])
        more = dot(w_high[0], p_high) + (dot(w_high[0], p_low) + dot(w_low[0], p_high))
        total = more if total is None else total + more
    width = total.shape[1] // splits
    for n, out in enumerate(outs):
        out[...] = total[:, n * width : (n + 1) * width]


def summed_products(turned, first, panels, start, splits):
    count = len(panels)
    _, height, depth = turned[0].shape
    width = panels[0].shape[1]
    tile = min(512, height)

    def weight_spec(n):
        return pl.BlockSpec((1, tile, depth), lambda m: (first + n, m, 0))

    in_specs = [weight_spec(n) for n in range(count)] * 2
    in_specs += [pl.BlockSpec((depth, width), lambda m: (0, 0))] * count
    operands = [turned[0]] * count + [turned[1]] * count + list(panels)
    if start is not None:
        in_specs.append(pl.BlockSpec((tile, width), lambda m: (m, 0)))
        operands.append(start)
    shape = jax.ShapeDtypeStruct((height, width // splits), jnp.float32)
    spec = pl.BlockSpec((tile, width // splits), lambda m: (m, 0))
    return pl.pallas_call(
        functools.partial(product_kernel, count, start is not None, splits),
        grid=(height // tile,),
        in_specs=in_specs,
        out_specs=[spec] * splits,
        out_shape=[shape] * splits,
        cost_estimate=pl.CostEstimate(
            flops=6 * count * depth * height * width,
            bytes_accessed=4 * (count * depth * (height + width) + 2 * height * width),
            transcendentals=0,
        ),
        name="summed_products",
    )(*operands)


def local(
    amplitudes, interaction, tile_counts, tile_block, recouple_sign, orbit_perm, particle_energy
):
    column = lax.axis_index("col")
    row = lax.axis_index("row")
    columns = lax.axis_size("col")
    rows = lax.axis_size("row")
    depth, across = grid_of(columns)
    slots, tile_rows, narrow = amplitudes.shape
    row_blocks = interaction.shape[0] // tile_rows
    col_blocks = interaction.shape[1] // tile_rows
    tile_total = tile_block.shape[0]
    piece = tile_rows // columns
    order = halving_order(rows)

    slot_ids = jnp.arange(slots, dtype=jnp.int32)
    is_live = slot_ids < jnp.take(tile_counts, column, mode="clip")
    own_block = lax.dynamic_slice_in_dim(tile_block, column * slots, slots)
    own_phase = 1 - 2 * lax.dynamic_slice_in_dim(recouple_sign, column * slots, slots)
    own_perm = lax.dynamic_slice_in_dim(orbit_perm, column * slots, slots, 0)
    tile_ids = jnp.arange(tile_total, dtype=jnp.int32)

    def tiles_of(blocks):
        matches = tile_block[None, :] == blocks[:, None]
        return jnp.sum(jnp.where(matches, tile_ids[None, :], 0), axis=1)

    orbitals = jnp.arange(tile_rows, dtype=jnp.int32)
    recouple = jnp.where(
        own_perm[:, :, None] == orbitals[None, None, :], own_phase[:, None, None], 0
    ).astype(jnp.float32)

    weights = interaction.reshape(row_blocks, columns, piece, interaction.shape[1])
    x = column % across
    picks = {}
    for mask in order:
        blocks = (row ^ mask) * row_blocks + jnp.arange(row_blocks, dtype=jnp.int32)
        picks[mask] = tiles_of(blocks)
    my_blocks = column * col_blocks + jnp.arange(col_blocks, dtype=jnp.int32)
    owners = tiles_of(my_blocks) // slots
    peers = jnp.arange(columns, dtype=jnp.int32)
    choice = jnp.sum(
        jnp.where(
            owners[None, :] == peers[:, None], jnp.arange(col_blocks, dtype=jnp.int32)[None, :], 0
        ),
        axis=1,
    )
    source = jnp.clip(own_block // col_blocks, 0, columns - 1)
    line = Line(depth, across)

    cut = jnp.einsum("sjp,spn->sjn", recouple, amplitudes, precision=lax.Precision.HIGHEST)
    cut = cut.reshape(slots, columns, piece, narrow).transpose(1, 0, 2, 3)
    cut = exchange(cut).reshape(tile_total, piece, narrow)

    def regroup(cut):
        parts = []
        for mask in order:
            part = jnp.take(cut, picks[mask], axis=0, mode="clip")
            if mask:
                part = lax.ppermute(part, "row", xor_pairs(rows, mask))
            parts.append(part.reshape(row_blocks * piece, cut.shape[2]))
        return jnp.concatenate(parts, axis=1)

    def across_x(held, mask):
        links = [
            (a * across + b, a * across + (b ^ mask)) for a in range(depth) for b in range(across)
        ]
        return lax.ppermute(held, "col", links)

    def crossed(held):
        return [
            [(value if mask == 0 else across_x(value, mask), z, mask) for mask in range(across)]
            for value, z in held
        ]

    ways = [(n, 0) for n in range(depth)] + [(n, m) for n in range(depth) for m in range(1, across)]
    ways.sort(key=lambda way: (way[0] + 2 * way[1], way[1]) if way[1] else (way[0] + 1, 0))
    index = jnp.stack([line.sources()[n] * across + (x ^ mask) for n, mask in ways])
    turned = turned_weights(weights, index)

    def product(panels):
        values = [panels[n][mask][0] for n, mask in ways]
        total, first = None, 0
        early = len(values) - max(1, len(values) // 4)
        for name, size in (("a", early), ("c", len(values) - early)):
            last = name == "c"
            out = summed_products(
                turned, first, values[first : first + size], total, 2 if last else 1,
            )
            total, first = out[0], first + size
        return out

    def to_row(value, bit):
        return lax.ppermute(value, "row", xor_pairs(rows, bit))

    def returned(home, tiles):
        picked = jnp.take(home, source, axis=0, mode="clip")
        back = jnp.einsum("sjp,sjn->spn", recouple, picked, precision=lax.Precision.HIGHEST)
        sigma = back + particle_energy[:, :, None] * tiles
        return jnp.where(is_live[:, None, None], sigma, 0.0)

    def halved(kept, arrived):
        width = kept.shape[1] // 2
        return kept[:, :width] + arrived[:, :width], kept[:, width:] + arrived[:, width:]

    chunks = max(1, narrow // 128)
    step = narrow // chunks
    tiles = [amplitudes[:, :, k * step : (k + 1) * step] for k in range(chunks)]
    outs = []
    panels, homes = [None] * chunks, [None] * chunks
    for k in range(chunks):
        shard = regroup(cut[:, :, k * step : (k + 1) * step])
        panels[k] = crossed(line.gather(shard))
    for k in range(chunks):
        kept, sent = product(panels[k])
        bit = 1
        while True:
            arrived = to_row(sent, bit)
            bit *= 2
            if bit >= rows:
                break
            kept, sent = halved(kept, arrived)
        if k:
            arrived = after(arrived, own)
        own = kept + arrived
        here = own.reshape(col_blocks, tile_rows, own.shape[1])

        homes[k] = exchange(jnp.take(here, choice, axis=0, mode="clip"))
        if k:
            outs.append(returned(after(homes[k - 1], sent), tiles[k - 1]))
    outs.append(returned(homes[-1], tiles[-1]))
    return jnp.concatenate(outs, axis=2)


def solution(mesh):
    placed = (P("col", None, "row"), P("row", "col"), P(), P(), P(), P(), P("col", None))

    return jax.shard_map(
        local, mesh=mesh, in_specs=placed, out_specs=P("col", None, "row"), check_vma=False
    )
```

```python
import functools

import jax
import jax.numpy as jnp
from jax import lax
from jax.experimental import pallas as pl
from jax.experimental.pallas import tpu as pltpu
from jax.sharding import PartitionSpec as P


def xor_pairs(count, mask):
    return [(i, i ^ mask) for i in range(count)]


def halving_order(count):
    order, bit = [0], count // 2
    while bit >= 1:
        order = order + [entry ^ bit for entry in order]
        bit //= 2
    return order


def grid_of(columns):
    across = 1
    while across * across * 4 <= columns:
        across *= 2
    return columns // across, across


def exchange(tiles):
    return lax.all_to_all(tiles, "col", split_axis=0, concat_axis=0, tiled=True)


def after(value, *others):
    return lax.optimization_barrier((value, *others))[0]


class Line:
    def __init__(self, depth, across):
        self.depth, self.across = depth, across
        self.z = lax.axis_index("col") // across

    def hop(self, value, pairs):
        links = [
            (a * self.across + x, b * self.across + x) for a, b in pairs for x in range(self.across)
        ]
        return lax.ppermute(value, "col", links)

    def sources(self):
        z, depth = self.z, self.depth
        if depth != 4:
            return [z] + [(z + depth - step) % depth for step in range(1, depth)]
        low = z < 2
        return [z, z ^ 1, jnp.where(low, 2, 1), jnp.where(low, 3, 0)]

    def gather(self, own):
        z, depth = self.z, self.depth
        if depth != 4:
            out = [(own, z)]
            for step in range(1, depth):
                pairs = [(a, (a + step) % depth) for a in range(depth)]
                out.append((self.hop(own, pairs), (z + depth - step) % depth))
            return out
        inner, low = jnp.logical_or(z == 1, z == 2), z < 2
        from_pair = self.hop(own, [(0, 1), (1, 0), (2, 3), (3, 2)])
        from_middle = self.hop(own, [(1, 2), (2, 1)])
        from_far_end = self.hop(from_pair, [(1, 2), (2, 1)])
        outward_near = self.hop(from_middle, [(1, 0), (2, 3)])
        outward_far = self.hop(from_far_end, [(1, 0), (2, 3)])
        second = jnp.where(inner, from_middle, outward_near)
        third = jnp.where(inner, from_far_end, outward_far)
        return [
            (own, z),
            (from_pair, z ^ 1),
            (second, jnp.where(low, 2, 1)),
            (third, jnp.where(low, 3, 0)),
        ]


def halves(value):
    high = value.astype(jnp.bfloat16)
    return high, (value - high.astype(jnp.float32)).astype(jnp.bfloat16)


def inbound_kernel(count, table, perm, tiles, energy, *rest):
    homes, (out, buffer, semaphores) = rest[:count], rest[-3:]
    slots, size, _ = buffer.shape

    def copy(source, slot):
        return pltpu.make_async_copy(source, buffer.at[slot], semaphores.at[slot])

    for slot in range(slots):
        if count == 1:
            copy(homes[0].at[table[0, slot]], slot).start()
        else:
            for n, home in enumerate(homes):
                pl.when(table[0, slot] == n)(lambda home=home: copy(home.at[0], slot).start())
    orbital = lax.broadcasted_iota(jnp.int32, (size, size), 0)
    for slot in range(slots):
        sign = table[1, slot].astype(jnp.float32)
        one_hot = jnp.where(perm[slot] == orbital, sign, 0.0).astype(jnp.bfloat16)
        copy(homes[0].at[0], slot).wait()
        values = buffer[slot]
        high, _ = halves(values)
        middle, low = halves(values - high.astype(jnp.float32))
        moved = [
            jnp.dot(one_hot, part, preferred_element_type=jnp.float32)
            for part in (high, middle, low)
        ]
        sigma = moved[0] + moved[1] + moved[2] + energy[slot] * tiles[slot]
        out[slot] = jnp.where(table[2, slot] > 0, sigma, 0.0)


def inbound(table, perm, homes, tiles, energy, chunk, before):
    slots, size, total = tiles.shape
    width = homes[0].shape[2]

    def here(n, table):
        return (0, 0, chunk)

    def whole(n, table):
        return (0, 0, 0)

    in_specs = [
        pl.BlockSpec((slots, 1, size), whole),
        pl.BlockSpec((slots, size, width), here),
        pl.BlockSpec((slots, size, 1), whole),
    ] + [pl.BlockSpec(memory_space=pl.ANY)] * len(homes)
    operands = [table, perm[:, None, :], tiles, energy[:, :, None], *homes]
    aliases = {}
    if before is not None:
        in_specs.append(pl.BlockSpec(memory_space=pl.ANY))
        aliases = {len(operands): 0}
        operands.append(before)
    return pl.pallas_call(
        functools.partial(inbound_kernel, len(homes)),
        grid_spec=pltpu.PrefetchScalarGridSpec(
            num_scalar_prefetch=1,
            grid=(1,),
            in_specs=in_specs,
            out_specs=pl.BlockSpec((slots, size, width), here),
            scratch_shapes=[
                pltpu.VMEM((slots, size, width), jnp.float32),
                pltpu.SemaphoreType.DMA((slots,)),
            ],
        ),
        out_shape=jax.ShapeDtypeStruct((slots, size, total), jnp.float32),
        input_output_aliases=aliases,
        name="inbound",
    )(*operands)


def weights_kernel(index, weight, high, low):
    del index
    rows = weight.shape[0] * weight.shape[2]
    high[0], low[0] = halves(weight[...].reshape(rows, weight.shape[3]).T)


def turned_weights(weights, index):
    groups, _, piece, height = weights.shape
    tile, count = min(512, height), index.shape[0]
    shape = jax.ShapeDtypeStruct((count, height, groups * piece), jnp.bfloat16)
    spec = pl.BlockSpec((1, tile, groups * piece), lambda k, m, index: (k, m, 0))
    return pl.pallas_call(
        weights_kernel,
        grid_spec=pltpu.PrefetchScalarGridSpec(
            num_scalar_prefetch=1,
            grid=(count, height // tile),
            in_specs=[
                pl.BlockSpec(
                    (groups, 1, piece, tile), lambda k, m, index: (0, index[k], 0, m)
                )
            ],
            out_specs=[spec, spec],
        ),
        out_shape=[shape, shape],
        cost_estimate=pl.CostEstimate(
            flops=20 * count * groups * piece * height * 100,
            bytes_accessed=8 * count * groups * piece * height,
            transcendentals=0,
        ),
        name="turned_weights",
    )(index, weights)


def product_kernel(count, has_start, splits, *refs):
    high, low, panels = refs[:count], refs[count : 2 * count], refs[2 * count : 3 * count]
    rest = refs[3 * count :]
    outs = rest[1:] if has_start else rest
    total = rest[0][...] if has_start else None

    def dot(a, b):
        return jnp.dot(a, b, preferred_element_type=jnp.float32)

    for w_high, w_low, panel in zip(high, low, panels):
        p_high, p_low = halves(panel[...])
        more = dot(w_high[0], p_high) + (dot(w_high[0], p_low) + dot(w_low[0], p_high))
        total = more if total is None else total + more
    width = total.shape[1] // splits
    for n, out in enumerate(outs):
        out[...] = total[:, n * width : (n + 1) * width]


def summed_products(turned, first, panels, start, splits):
    count = len(panels)
    _, height, depth = turned[0].shape
    width = panels[0].shape[1]
    tile = min(512, height)

    def weight_spec(n):
        return pl.BlockSpec((1, tile, depth), lambda m: (first + n, m, 0))

    in_specs = [weight_spec(n) for n in range(count)] * 2
    in_specs += [pl.BlockSpec((depth, width), lambda m: (0, 0))] * count
    operands = [turned[0]] * count + [turned[1]] * count + list(panels)
    if start is not None:
        in_specs.append(pl.BlockSpec((tile, width), lambda m: (m, 0)))
        operands.append(start)
    shape = jax.ShapeDtypeStruct((height, width // splits), jnp.float32)
    spec = pl.BlockSpec((tile, width // splits), lambda m: (m, 0))
    return pl.pallas_call(
        functools.partial(product_kernel, count, start is not None, splits),
        grid=(height // tile,),
        in_specs=in_specs,
        out_specs=[spec] * splits,
        out_shape=[shape] * splits,
        cost_estimate=pl.CostEstimate(
            flops=6 * count * depth * height * width,
            bytes_accessed=4 * (count * depth * (height + width) + 2 * height * width),
            transcendentals=0,
        ),
        name="summed_products",
    )(*operands)


def local(
    amplitudes, interaction, tile_counts, tile_block, recouple_sign, orbit_perm, particle_energy
):
    column = lax.axis_index("col")
    row = lax.axis_index("row")
    columns = lax.axis_size("col")
    rows = lax.axis_size("row")
    depth, across = grid_of(columns)
    slots, tile_rows, narrow = amplitudes.shape
    row_blocks = interaction.shape[0] // tile_rows
    col_blocks = interaction.shape[1] // tile_rows
    tile_total = tile_block.shape[0]
    piece = tile_rows // columns
    order = halving_order(rows)

    slot_ids = jnp.arange(slots, dtype=jnp.int32)
    is_live = slot_ids < jnp.take(tile_counts, column, mode="clip")
    own_block = lax.dynamic_slice_in_dim(tile_block, column * slots, slots)
    own_phase = 1 - 2 * lax.dynamic_slice_in_dim(recouple_sign, column * slots, slots)
    own_perm = lax.dynamic_slice_in_dim(orbit_perm, column * slots, slots, 0)
    tile_ids = jnp.arange(tile_total, dtype=jnp.int32)

    def tiles_of(blocks):
        matches = tile_block[None, :] == blocks[:, None]
        return jnp.sum(jnp.where(matches, tile_ids[None, :], 0), axis=1)

    orbitals = jnp.arange(tile_rows, dtype=jnp.int32)
    recouple = jnp.where(
        own_perm[:, :, None] == orbitals[None, None, :], own_phase[:, None, None], 0
    ).astype(jnp.float32)

    weights = interaction.reshape(row_blocks, columns, piece, interaction.shape[1])
    x = column % across
    picks = {}
    for mask in order:
        blocks = (row ^ mask) * row_blocks + jnp.arange(row_blocks, dtype=jnp.int32)
        picks[mask] = tiles_of(blocks)
    my_blocks = column * col_blocks + jnp.arange(col_blocks, dtype=jnp.int32)
    owners = tiles_of(my_blocks) // slots
    peers = jnp.arange(columns, dtype=jnp.int32)
    choice = jnp.sum(
        jnp.where(
            owners[None, :] == peers[:, None], jnp.arange(col_blocks, dtype=jnp.int32)[None, :], 0
        ),
        axis=1,
    )
    source = jnp.clip(own_block // col_blocks, 0, columns - 1)
    line = Line(depth, across)

    cut = jnp.einsum("sjp,spn->sjn", recouple, amplitudes, precision=lax.Precision.HIGHEST)
    cut = cut.reshape(slots, columns, piece, narrow).transpose(1, 0, 2, 3)
    cut = exchange(cut).reshape(tile_total, piece, narrow)

    def regroup(cut):
        parts = []
        for mask in order:
            part = jnp.take(cut, picks[mask], axis=0, mode="clip")
            if mask:
                part = lax.ppermute(part, "row", xor_pairs(rows, mask))
            parts.append(part.reshape(row_blocks * piece, cut.shape[2]))
        return jnp.concatenate(parts, axis=1)

    def across_x(held, mask):
        links = [
            (a * across + b, a * across + (b ^ mask)) for a in range(depth) for b in range(across)
        ]
        return lax.ppermute(held, "col", links)

    def crossed(held):
        return [
            [(value if mask == 0 else across_x(value, mask), z, mask) for mask in range(across)]
            for value, z in held
        ]

    ways = [(n, 0) for n in range(depth)] + [(n, m) for n in range(depth) for m in range(1, across)]
    ways.sort(key=lambda way: (way[0] + 2 * way[1], way[1]) if way[1] else (way[0] + 1, 0))
    index = jnp.stack([line.sources()[n] * across + (x ^ mask) for n, mask in ways])
    turned = turned_weights(weights, index)

    final_weight = lax.dynamic_slice_in_dim(weights, index[-1], 1, 1)
    final_weight = final_weight.reshape(row_blocks * piece, interaction.shape[1])

    def last_product(panel):
        return lax.dot_general(
            final_weight,
            panel,
            (((0,), (0,)), ((), ())),
            precision=lax.Precision.HIGH,
            preferred_element_type=jnp.float32,
        )

    def product(panels):
        values = [panels[n][mask][0] for n, mask in ways]
        (total,) = summed_products(turned, 0, values[:-1], None, 1)
        width = total.shape[1] // 2
        sent = total[:, width:] + last_product(values[-1][:, width:])
        return total[:, :width] + last_product(values[-1][:, :width]), sent

    def to_row(value, bit):
        return lax.ppermute(value, "row", xor_pairs(rows, bit))

    def halved(kept, arrived):
        width = kept.shape[1] // 2
        return kept[:, :width] + arrived[:, :width], kept[:, width:] + arrived[:, width:]

    chunks = max(1, narrow // 128)
    step = narrow // chunks
    sigma = None
    live = is_live.astype(jnp.int32)
    panels, homes = [None] * chunks, [None] * chunks
    for k in range(chunks):
        shard = regroup(cut[:, :, k * step : (k + 1) * step])
        panels[k] = crossed(line.gather(shard))
    for k in range(chunks):
        kept, sent = product(panels[k])
        bit = 1
        while True:
            arrived = to_row(sent, bit)
            bit *= 2
            if bit >= rows:
                break
            kept, sent = halved(kept, arrived)
        if k:
            arrived = after(arrived, own)
        own = kept + arrived
        here = own.reshape(col_blocks, tile_rows, own.shape[1])

        last = k + 1 == chunks
        if last:
            mine = jnp.take(here, jnp.take(choice, column ^ peers, mode="clip"), axis=0, mode="clip")
            blocks = [mine[mask : mask + 1] for mask in range(columns)]
            for mask in FARTHEST if columns == len(FARTHEST) + 1 else range(1, columns):
                blocks[mask] = lax.ppermute(blocks[mask], "col", xor_pairs(columns, mask))
            homes[k] = blocks
        else:
            homes[k] = [exchange(jnp.take(here, choice, axis=0, mode="clip"))]
        if k:
            table = jnp.stack([source, own_phase, live])
            homes[k - 1][0] = after(homes[k - 1][0], sent)
            sigma = inbound(
                table, own_perm, homes[k - 1], amplitudes, particle_energy, k - 1, sigma
            )
    table = jnp.stack([source ^ column, own_phase, live])
    return inbound(table, own_perm, homes[-1], amplitudes, particle_energy, chunks - 1, sigma)


FARTHEST = (6, 7, 4, 5, 2, 3, 1)


def solution(mesh):
    placed = (P("col", None, "row"), P("row", "col"), P(), P(), P(), P(), P("col", None))

    return jax.shard_map(
        local, mesh=mesh, in_specs=placed, out_specs=P("col", None, "row"), check_vma=False
    )
```

```python
import functools

import jax
import jax.numpy as jnp
from jax import lax
from jax.experimental import pallas as pl
from jax.experimental.pallas import tpu as pltpu
from jax.sharding import PartitionSpec as P


def xor_pairs(count, mask):
    return [(i, i ^ mask) for i in range(count)]


def halving_order(count):
    order, bit = [0], count // 2
    while bit >= 1:
        order = order + [entry ^ bit for entry in order]
        bit //= 2
    return order


def grid_of(columns):
    across = 1
    while across * across * 4 <= columns:
        across *= 2
    return columns // across, across


def exchange(tiles):
    return lax.all_to_all(tiles, "col", split_axis=0, concat_axis=0, tiled=True)


def after(value, *others):
    return lax.optimization_barrier((value, *others))[0]


class Line:
    def __init__(self, depth, across):
        self.depth, self.across = depth, across
        self.z = lax.axis_index("col") // across

    def hop(self, value, pairs):
        links = [
            (a * self.across + x, b * self.across + x) for a, b in pairs for x in range(self.across)
        ]
        return lax.ppermute(value, "col", links)

    def sources(self):
        z, depth = self.z, self.depth
        if depth != 4:
            return [z] + [(z + depth - step) % depth for step in range(1, depth)]
        low = z < 2
        return [z, z ^ 1, jnp.where(low, 2, 1), jnp.where(low, 3, 0)]

    def gather(self, own):
        z, depth = self.z, self.depth
        if depth != 4:
            out = [(own, z)]
            for step in range(1, depth):
                pairs = [(a, (a + step) % depth) for a in range(depth)]
                out.append((self.hop(own, pairs), (z + depth - step) % depth))
            return out
        inner, low = jnp.logical_or(z == 1, z == 2), z < 2
        from_pair = self.hop(own, [(0, 1), (1, 0), (2, 3), (3, 2)])
        from_middle = self.hop(own, [(1, 2), (2, 1)])
        from_far_end = self.hop(from_pair, [(1, 2), (2, 1)])
        outward_near = self.hop(from_middle, [(1, 0), (2, 3)])
        outward_far = self.hop(from_far_end, [(1, 0), (2, 3)])
        second = jnp.where(inner, from_middle, outward_near)
        third = jnp.where(inner, from_far_end, outward_far)
        return [
            (own, z),
            (from_pair, z ^ 1),
            (second, jnp.where(low, 2, 1)),
            (third, jnp.where(low, 3, 0)),
        ]


def halves(value):
    high = value.astype(jnp.bfloat16)
    return high, (value - high.astype(jnp.float32)).astype(jnp.bfloat16)


def inbound_kernel(count, table, perm, tiles, energy, *rest):
    homes, (out, buffer, semaphores) = rest[:count], rest[-3:]
    slots, size, _ = buffer.shape

    def copy(source, slot):
        return pltpu.make_async_copy(source, buffer.at[slot], semaphores.at[slot])

    for slot in range(slots):
        if count == 1:
            copy(homes[0].at[table[0, slot]], slot).start()
        else:
            for n, home in enumerate(homes):
                pl.when(table[0, slot] == n)(lambda home=home: copy(home.at[0], slot).start())
    orbital = lax.broadcasted_iota(jnp.int32, (size, size), 0)
    for slot in range(slots):
        sign = table[1, slot].astype(jnp.float32)
        one_hot = jnp.where(perm[slot] == orbital, sign, 0.0).astype(jnp.bfloat16)
        copy(homes[0].at[0], slot).wait()
        values = buffer[slot]
        high, _ = halves(values)
        middle, low = halves(values - high.astype(jnp.float32))
        moved = [
            jnp.dot(one_hot, part, preferred_element_type=jnp.float32)
            for part in (high, middle, low)
        ]
        sigma = moved[0] + moved[1] + moved[2] + energy[slot] * tiles[slot]
        out[slot] = jnp.where(table[2, slot] > 0, sigma, 0.0)


def inbound(table, perm, homes, tiles, energy, chunk, before):
    slots, size, total = tiles.shape
    width = homes[0].shape[2]

    def here(n, table):
        return (0, 0, chunk)

    def whole(n, table):
        return (0, 0, 0)

    in_specs = [
        pl.BlockSpec((slots, 1, size), whole),
        pl.BlockSpec((slots, size, width), here),
        pl.BlockSpec((slots, size, 1), whole),
    ] + [pl.BlockSpec(memory_space=pl.ANY)] * len(homes)
    operands = [table, perm[:, None, :], tiles, energy[:, :, None], *homes]
    aliases = {}
    if before is not None:
        in_specs.append(pl.BlockSpec(memory_space=pl.ANY))
        aliases = {len(operands): 0}
        operands.append(before)
    return pl.pallas_call(
        functools.partial(inbound_kernel, len(homes)),
        grid_spec=pltpu.PrefetchScalarGridSpec(
            num_scalar_prefetch=1,
            grid=(1,),
            in_specs=in_specs,
            out_specs=pl.BlockSpec((slots, size, width), here),
            scratch_shapes=[
                pltpu.VMEM((slots, size, width), jnp.float32),
                pltpu.SemaphoreType.DMA((slots,)),
            ],
        ),
        out_shape=jax.ShapeDtypeStruct((slots, size, total), jnp.float32),
        input_output_aliases=aliases,
        name="inbound",
    )(*operands)


def weights_kernel(index, weight, high, low):
    del index
    rows = weight.shape[0] * weight.shape[2]
    high[0], low[0] = halves(weight[...].reshape(rows, weight.shape[3]).T)


def turned_weights(weights, index):
    groups, _, piece, height = weights.shape
    tile, count = min(512, height), index.shape[0]
    shape = jax.ShapeDtypeStruct((count, height, groups * piece), jnp.bfloat16)
    spec = pl.BlockSpec((1, tile, groups * piece), lambda k, m, index: (k, m, 0))
    return pl.pallas_call(
        weights_kernel,
        grid_spec=pltpu.PrefetchScalarGridSpec(
            num_scalar_prefetch=1,
            grid=(count, height // tile),
            in_specs=[
                pl.BlockSpec(
                    (groups, 1, piece, tile), lambda k, m, index: (0, index[k], 0, m)
                )
            ],
            out_specs=[spec, spec],
        ),
        out_shape=[shape, shape],
        cost_estimate=pl.CostEstimate(
            flops=20 * count * groups * piece * height * 100,
            bytes_accessed=8 * count * groups * piece * height,
            transcendentals=0,
        ),
        name="turned_weights",
    )(index, weights)


def product_kernel(count, has_start, splits, *refs):
    high, low, panels = refs[:count], refs[count : 2 * count], refs[2 * count : 3 * count]
    rest = refs[3 * count :]
    outs = rest[1:] if has_start else rest
    total = rest[0][...] if has_start else None

    def dot(a, b):
        return jnp.dot(a, b, preferred_element_type=jnp.float32)

    for w_high, w_low, panel in zip(high, low, panels):
        p_high, p_low = halves(panel[...])
        more = dot(w_high[0], p_high) + (dot(w_high[0], p_low) + dot(w_low[0], p_high))
        total = more if total is None else total + more
    width = total.shape[1] // splits
    for n, out in enumerate(outs):
        out[...] = total[:, n * width : (n + 1) * width]


def summed_products(turned, first, panels, start, splits):
    count = len(panels)
    _, height, depth = turned[0].shape
    width = panels[0].shape[1]
    tile = min(512, height)

    def weight_spec(n):
        return pl.BlockSpec((1, tile, depth), lambda m: (first + n, m, 0))

    in_specs = [weight_spec(n) for n in range(count)] * 2
    in_specs += [pl.BlockSpec((depth, width), lambda m: (0, 0))] * count
    operands = [turned[0]] * count + [turned[1]] * count + list(panels)
    if start is not None:
        in_specs.append(pl.BlockSpec((tile, width), lambda m: (m, 0)))
        operands.append(start)
    shape = jax.ShapeDtypeStruct((height, width // splits), jnp.float32)
    spec = pl.BlockSpec((tile, width // splits), lambda m: (m, 0))
    return pl.pallas_call(
        functools.partial(product_kernel, count, start is not None, splits),
        grid=(height // tile,),
        in_specs=in_specs,
        out_specs=[spec] * splits,
        out_shape=[shape] * splits,
        cost_estimate=pl.CostEstimate(
            flops=6 * count * depth * height * width,
            bytes_accessed=4 * (count * depth * (height + width) + 2 * height * width),
            transcendentals=0,
        ),
        name="summed_products",
    )(*operands)


def local(
    amplitudes, interaction, tile_counts, tile_block, recouple_sign, orbit_perm, particle_energy
):
    column = lax.axis_index("col")
    row = lax.axis_index("row")
    columns = lax.axis_size("col")
    rows = lax.axis_size("row")
    depth, across = grid_of(columns)
    slots, tile_rows, narrow = amplitudes.shape
    row_blocks = interaction.shape[0] // tile_rows
    col_blocks = interaction.shape[1] // tile_rows
    tile_total = tile_block.shape[0]
    piece = tile_rows // columns
    order = halving_order(rows)

    slot_ids = jnp.arange(slots, dtype=jnp.int32)
    is_live = slot_ids < jnp.take(tile_counts, column, mode="clip")
    own_block = lax.dynamic_slice_in_dim(tile_block, column * slots, slots)
    own_phase = 1 - 2 * lax.dynamic_slice_in_dim(recouple_sign, column * slots, slots)
    own_perm = lax.dynamic_slice_in_dim(orbit_perm, column * slots, slots, 0)
    tile_ids = jnp.arange(tile_total, dtype=jnp.int32)

    def tiles_of(blocks):
        matches = tile_block[None, :] == blocks[:, None]
        return jnp.sum(jnp.where(matches, tile_ids[None, :], 0), axis=1)

    orbitals = jnp.arange(tile_rows, dtype=jnp.int32)
    recouple = jnp.where(
        own_perm[:, :, None] == orbitals[None, None, :], own_phase[:, None, None], 0
    ).astype(jnp.float32)

    weights = interaction.reshape(row_blocks, columns, piece, interaction.shape[1])
    x = column % across
    picks = {}
    for mask in order:
        blocks = (row ^ mask) * row_blocks + jnp.arange(row_blocks, dtype=jnp.int32)
        picks[mask] = tiles_of(blocks)
    my_blocks = column * col_blocks + jnp.arange(col_blocks, dtype=jnp.int32)
    owners = tiles_of(my_blocks) // slots
    peers = jnp.arange(columns, dtype=jnp.int32)
    choice = jnp.sum(
        jnp.where(
            owners[None, :] == peers[:, None], jnp.arange(col_blocks, dtype=jnp.int32)[None, :], 0
        ),
        axis=1,
    )
    source = jnp.clip(own_block // col_blocks, 0, columns - 1)
    line = Line(depth, across)

    cut = jnp.einsum("sjp,spn->sjn", recouple, amplitudes, precision=lax.Precision.HIGHEST)
    cut = cut.reshape(slots, columns, piece, narrow).transpose(1, 0, 2, 3)
    cut = exchange(cut).reshape(tile_total, piece, narrow)

    def regroup(cut):
        parts = []
        for mask in order:
            part = jnp.take(cut, picks[mask], axis=0, mode="clip")
            if mask:
                part = lax.ppermute(part, "row", xor_pairs(rows, mask))
            parts.append(part.reshape(row_blocks * piece, cut.shape[2]))
        return jnp.concatenate(parts, axis=1)

    def across_x(held, mask):
        links = [
            (a * across + b, a * across + (b ^ mask)) for a in range(depth) for b in range(across)
        ]
        return lax.ppermute(held, "col", links)

    def crossed(held):
        return [
            [(value if mask == 0 else across_x(value, mask), z, mask) for mask in range(across)]
            for value, z in held
        ]

    ways = [(n, 0) for n in range(depth)] + [(n, m) for n in range(depth) for m in range(1, across)]
    ways.sort(key=lambda way: (way[0] + 2 * way[1], way[1]) if way[1] else (way[0] + 1, 0))
    index = jnp.stack([line.sources()[n] * across + (x ^ mask) for n, mask in ways])
    turned = turned_weights(weights, index)

    final_weight = lax.dynamic_slice_in_dim(weights, index[-1], 1, 1)
    final_weight = final_weight.reshape(row_blocks * piece, interaction.shape[1])

    def last_product(panel):
        return lax.dot_general(
            final_weight,
            panel,
            (((0,), (0,)), ((), ())),
            precision=lax.Precision.HIGH,
            preferred_element_type=jnp.float32,
        )

    def product(panels, chunk):
        values = [panels[n][mask][0] for n, mask in ways]
        early = len(values) // 2 - chunk
        (total,) = summed_products(turned, 0, values[:early], None, 1)
        (total,) = summed_products(turned, early, values[early:-1], total, 1)
        width = total.shape[1] // 2
        sent = total[:, width:] + last_product(values[-1][:, width:])
        return total[:, :width] + last_product(values[-1][:, :width]), sent

    def to_row(value, bit):
        return lax.ppermute(value, "row", xor_pairs(rows, bit))

    def halved(kept, arrived):
        width = kept.shape[1] // 2
        return kept[:, :width] + arrived[:, :width], kept[:, width:] + arrived[:, width:]

    chunks = max(1, narrow // 128)
    step = narrow // chunks
    sigma = None
    live = is_live.astype(jnp.int32)
    panels, homes = [None] * chunks, [None] * chunks
    for k in range(chunks):
        shard = regroup(cut[:, :, k * step : (k + 1) * step])
        panels[k] = crossed(line.gather(shard))
    for k in range(chunks):
        kept, sent = product(panels[k], k)
        bit = 1
        while True:
            arrived = to_row(sent, bit)
            bit *= 2
            if bit >= rows:
                break
            kept, sent = halved(kept, arrived)
        if k:
            arrived = after(arrived, own)
        own = kept + arrived
        here = own.reshape(col_blocks, tile_rows, own.shape[1])

        last = k + 1 == chunks
        if last:
            mine = jnp.take(here, jnp.take(choice, column ^ peers, mode="clip"), axis=0, mode="clip")
            blocks = [mine[mask : mask + 1] for mask in range(columns)]
            for mask in FARTHEST if columns == len(FARTHEST) + 1 else range(1, columns):
                blocks[mask] = lax.ppermute(blocks[mask], "col", xor_pairs(columns, mask))
            homes[k] = blocks
        else:
            homes[k] = [exchange(jnp.take(here, choice, axis=0, mode="clip"))]
        if k:
            table = jnp.stack([source, own_phase, live])
            homes[k - 1][0] = after(homes[k - 1][0], sent)
            sigma = inbound(
                table, own_perm, homes[k - 1], amplitudes, particle_energy, k - 1, sigma
            )
    table = jnp.stack([source ^ column, own_phase, live])
    return inbound(table, own_perm, homes[-1], amplitudes, particle_energy, chunks - 1, sigma)


FARTHEST = (6, 7, 4, 5, 2, 3, 1)


def solution(mesh):
    placed = (P("col", None, "row"), P("row", "col"), P(), P(), P(), P(), P("col", None))

    return jax.shard_map(
        local, mesh=mesh, in_specs=placed, out_specs=P("col", None, "row"), check_vma=False
    )
```
